128 devices in a mesh: groups: 4 (over x, y), blk: 32 (over z, core).
Axes of the slice: x: 2, y: 2, z: 16, core: 2. Of those that a mesh axis runs over, the one named last changes fastest.
The devices are a block of a 8x8x16 slice.
Arguments:
- pair_elements: float32 [49152, 1024], P(('groups', 'blk')), parts along dimension 0, may hold values from -0.8 to 0.8
- gmap: int32 [49152], P(('groups', 'blk')), parts along dimension 0, may hold values from 0 to 12287, as said below
- w_screened: float32 [49152, 12288], P('groups', 'blk'), parts along dimension 0, as said below
- coulomb: float32 [49152], P(('groups', 'blk')), parts along dimension 0, may hold values from 0.001 to 0.02
Outputs:
- screened: float32 [49152, 1024], P(('groups', 'blk')), parts along dimension 0
- pair_sigma: float32 [4096], P(('groups', 'blk')), parts along dimension 0
The draws below stay inside these ranges and needn't reach their ends.
There are 4 independent parts, one for each index of `groups`. The reference program is written for one: setup_inputs(seed, part) draws one part's arguments, and reference() takes and returns one part's arrays. A program takes and returns all parts, laid end to end along the dimension named above; each array names one. Nothing has to cross between parts.
Inputs may be any that keep to these rules, and one draw needn't show every extreme that they name: `gmap`: each aligned block of 384 entries is a permutation of that block's own indices. `w_screened`: symmetric.
All inputs are finite; a program needn't handle non-finite values.
Results may differ from the reference program's by a relative error of at most 0.00013.
Values sent between devices are 32-bit elements; how exact they have to be, the bound alone decides.
A program may use at most 256 MiB of HBM per device.

```python
import math
import jax
import jax.numpy as jnp
from jax import lax

G_DEV = 384
NG = 12288
NB = 64
OCC = 4
P_SIZE = 1024


def draw_gmap(key, part):
    blocks = NG // G_DEV
    scores = jax.random.randint(key, (blocks, G_DEV), 0, 1 << 30)
    scores = scores * G_DEV + jnp.arange(G_DEV, dtype=jnp.int32)[None, :]
    order = jnp.argsort(scores, axis=1, stable=True).astype(jnp.int32)
    offsets = (jnp.arange(blocks, dtype=jnp.int32) * G_DEV)[:, None]
    return (order + offsets).reshape(NG).astype(jnp.int32)


def draw_w_screened(key, part):
    base = jax.random.normal(key, (NG, NG), jnp.float32)
    return ((base + base.T) * (0.5 / NG) ** 0.5).astype(jnp.float32)


def raised(entries, own_key, source, target, shards_of, factor):
    def block_of(dim):
        return (jnp.arange(entries.shape[dim]) // (entries.shape[dim] // shards_of)).reshape((-1,) + (1,) * (entries.ndim - 1 - dim))

    first = jax.random.permutation(own_key, shards_of)[block_of(target)]
    far = (block_of(target) + shards_of // 2) % shards_of
    return jnp.where((block_of(source) == first) | (block_of(source) == far), factor * entries, entries)


def steps_of(key, dims, shards, smallest, top_value):
    level, own = 1.0, jax.random.fold_in(key, 6)
    for axis_at, shards_of in shards:
        steps = jnp.exp(jax.random.uniform(jax.random.fold_in(own, axis_at), (shards_of,), jnp.float32, smallest / len(shards), top_value / len(shards)))
        level = level * jnp.repeat(steps, dims[axis_at] // shards_of).reshape([-1 if axis == axis_at else 1 for axis in range(len(dims))])
    return level


def noise_with(own_key, dims, deviation, reach, cuts, heavy, kind=jnp.bfloat16):
    result = deviation * jax.random.normal(own_key, dims, jnp.float32)
    if cuts:
        result = result * steps_of(own_key, dims, cuts, -0.22, 0.18)
    return jnp.clip(raised(result, jax.random.fold_in(own_key, 3), *heavy), -reach, reach).astype(kind)


def setup_inputs(seed: int = 0, part: int = 0) -> dict:
    key_list = jax.random.split(jax.random.key(seed), 5)
    part_keys = jax.random.split(jax.random.fold_in(key_list[4], part), 5)
    return {
        "pair_elements": noise_with(part_keys[0], (NG, P_SIZE), 0.1, 0.8, ((0, 32),), (0, 1, 32, 2.75), jnp.float32),
        "gmap": draw_gmap(jax.random.fold_in(jax.random.fold_in(key_list[4], part), 71), part),
        "w_screened": draw_w_screened(jax.random.fold_in(jax.random.fold_in(key_list[4], part), 71), part),
        "coulomb": jnp.clip(jnp.exp(math.log(0.02) - 2.9957322 * jax.random.uniform(part_keys[3], (NG,), jnp.float32) ** steps_of(part_keys[3], (NG,), ((0, 32),), -0.2, 0.2)), 0.001, 0.02),
    }


def reference(pair_elements, gmap, w_screened, coulomb):
    elements = jnp.take(pair_elements, gmap.astype(jnp.int32), axis=0)
    screened = lax.dot_general(w_screened, elements, (((0,), (0,)), ((), ())), precision=lax.Precision.HIGHEST, preferred_element_type=jnp.float32)
    band = jnp.arange(P_SIZE, dtype=jnp.int32) % NB
    coef = jnp.where(band < OCC, -0.5, 0.5).astype(jnp.float32)
    pair_sigma = coef * jnp.sum(screened * elements, axis=0) - 0.5 * jnp.sum(coulomb[:, None] * elements * elements, axis=0)
    return screened, pair_sigma
```

```python
import functools

import jax
import jax.numpy as jnp
from jax import lax
from jax.experimental import pallas as pl
from jax.experimental.pallas import tpu as pltpu
from jax.sharding import PartitionSpec as P

NB = 64
OCC = 4
TILES = 4
MESH = pl.DeviceIdType.MESH


def split(x):
    hi = x.astype(jnp.bfloat16)
    return hi, (x - hi.astype(jnp.float32)).astype(jnp.bfloat16)


def dot(a, b):
    return jnp.dot(a, b, preferred_element_type=jnp.float32)


def kernel(
    devices,
    e_ref, w_ref, v_ref, out_ref, sig_ref,
    buf, wbuf, wt_hi, wt_lo, bare, terms, landed,
    ring_recv, pair_recv, right_send, left_send, pair_send, local_sem, w_sem, term_send, term_recv,
):
    rows, pairs = e_ref.shape
    width = pairs // TILES
    depth = devices // 2
    half = depth // 2
    group, me = lax.axis_index("groups"), lax.axis_index("blk")
    z, core = me // 2, me % 2

    def at(blk):
        return (group, blk)

    right = at(lax.rem(z + 1, depth) * 2 + core)
    left = at(lax.rem(z + depth - 1, depth) * 2 + core)
    partner = at(z * 2 + 1 - core)

    barrier = pltpu.get_barrier_semaphore()
    for other in (right, left, partner):
        pl.semaphore_signal(barrier, inc=1, device_id=other, device_id_type=MESH)

    def w_copy(i, block):
        source = pl.ds(pl.multiple_of(block * 2 * rows, 2 * rows), 2 * rows)
        return pltpu.make_async_copy(w_ref.at[source, :], wbuf.at[i % 2], w_sem.at[i % 2])

    def behind(s):
        return lax.rem(z + depth - s, depth)

    def ahead(s):
        return lax.rem(z + s, depth)

    def piece(source, which, k):
        start = pl.multiple_of((source * 2 + which) * rows, rows)
        return buf.at[k, pl.ds(start, rows), :]

    own_piece = [e_ref.at[:, pl.ds(k * width, width)] for k in range(TILES)]

    def ring_copy(src, source, k, send_sem, device):
        return pltpu.make_async_remote_copy(
            src_ref=src, dst_ref=piece(source, core, k), send_sem=send_sem.at[0],
            recv_sem=ring_recv.at[source, k], device_id=device, device_id_type=MESH)

    def pair_copy(src, source, which, k):
        return pltpu.make_async_remote_copy(
            src_ref=src, dst_ref=piece(source, which, k), send_sem=pair_send.at[0],
            recv_sem=pair_recv.at[source, k], device_id=partner, device_id_type=MESH)

    w_copy(0, z).start()
    w_copy(1, behind(1)).start()
    for k in range(TILES):
        pltpu.make_async_copy(own_piece[k], piece(z, core, k), local_sem.at[k]).start()
    pl.semaphore_wait(barrier, 3)
    for k in range(TILES):
        ring_copy(own_piece[k], z, k, right_send, right).start()
        ring_copy(own_piece[k], z, k, left_send, left).start()
        pair_copy(own_piece[k], z, core, k).start()

    def load_w(i, block):
        w_copy(i, block).wait()
        for part in range(2):
            cols = slice(part * rows, part * rows + rows)
            hi, lo = split(jnp.transpose(wbuf[i % 2, cols, :]))
            wt_hi[:, cols] = hi
            wt_lo[:, cols] = lo

    def product(k, block):
        start = pl.multiple_of(block * 2 * rows, 2 * rows)
        hi, lo = split(buf[k, pl.ds(start, 2 * rows), :])
        return dot(wt_hi[...], hi) + (dot(wt_hi[...], lo) + dot(wt_lo[...], hi))

    def tile(k):
        return pl.ds(pl.multiple_of(k * width, width), width)

    def add_block(block):
        def body(k, carry):
            out_ref[:, tile(k)] += product(k, block)
            return carry

        lax.fori_loop(0, TILES, body, 0)

    def pass_on(source, k, send_sem, device, onward):
        copy = ring_copy(piece(source, core, k), source, k, send_sem, device)
        copy.wait_recv()
        if onward is True:
            copy.start()
        elif onward is not False:
            pl.when(onward)(copy.start)
        pair_copy(piece(source, core, k), source, core, k).start()

    def take_pair(source, k):
        pair_copy(piece(source, 1 - core, k), source, 1 - core, k).wait_recv()

    load_w(0, z)
    w_copy(2, ahead(1)).start()
    for k in range(TILES):
        pltpu.make_async_copy(own_piece[k], piece(z, core, k), local_sem.at[k]).wait()
        take_pair(z, k)

    def first(k, carry):
        out_ref[:, tile(k)] = product(k, z)
        own = buf[k, pl.ds(pl.multiple_of(me * rows, rows), rows), :]
        bare[k] = jnp.dot(v_ref[...], own * own, precision=lax.Precision.HIGHEST, preferred_element_type=jnp.float32)
        return carry

    lax.fori_loop(0, TILES, first, 0)

    def step(s, carry):
        for k in range(TILES):
            on_right = True if k < TILES // 2 else s < half - 1
            on_left = True if k >= TILES // 2 else s < half - 1
            pass_on(behind(s), k, right_send, right, on_right)
            pass_on(ahead(s), k, left_send, left, on_left)
        load_w(1, behind(s))
        w_copy(1, behind(s + 1)).start()
        for k in range(TILES):
            take_pair(behind(s), k)
        add_block(behind(s))
        load_w(0, ahead(s))

        @pl.when(s < half - 1)
        def _():
            w_copy(0, ahead(s + 1)).start()

        for k in range(TILES):
            take_pair(ahead(s), k)
        add_block(ahead(s))
        return carry

    lax.fori_loop(1, half, step, 0)

    last = behind(half)
    load_w(1, last)
    lanes = terms.shape[-1]
    per_owner = pairs // devices
    owners_per_row = lanes // per_owner
    for j in range(TILES // 2):
        both = (j, TILES // 2 + j)
        pass_on(last, both[0], right_send, right, False)
        pass_on(last, both[1], left_send, left, False)
        for k in both:
            take_pair(last, k)
            cols = slice(k * width, (k + 1) * width)
            screened = out_ref[:, cols] + product(k, last)
            out_ref[:, cols] = screened
            own = buf[k, pl.ds(pl.multiple_of(me * rows, rows), rows), :]
            pair = lax.broadcasted_iota(jnp.int32, (1, width), 1) + k * width
            coef = jnp.where(pair % NB < OCC, -0.5, 0.5).astype(jnp.float32)
            term = coef * jnp.sum(screened * own, axis=0, keepdims=True) - 0.5 * bare[k]
            for r in range(width // lanes):
                terms[k * width // lanes + r] = term[:, r * lanes : (r + 1) * lanes]

    def term_copy(owner, slot):
        return pltpu.make_async_remote_copy(
            src_ref=terms.at[owner // owners_per_row], dst_ref=landed.at[slot], send_sem=term_send.at[0],
            recv_sem=term_recv.at[0], device_id=at(owner), device_id_type=MESH)

    def send_term(n, carry):
        owner = lax.rem(me + n, devices)
        term_copy(owner, lax.rem(me - owner - 1 + devices, devices)).start()
        return carry

    lax.fori_loop(1, devices, send_term, 0)

    whole = pltpu.make_async_copy(landed, landed, term_recv.at[0])
    whole.wait()
    total = terms[me // owners_per_row] + jnp.sum(landed[...], axis=0)
    place = me % owners_per_row
    mine = total[:, :per_owner]
    for r in range(1, owners_per_row):
        mine = jnp.where(place == r, total[:, r * per_owner : (r + 1) * per_owner], mine)
    sig_ref[...] = mine

    sent = pl.ds(0, (half - 1) * rows + rows // 2)
    for sem in (right_send, left_send):
        pltpu.make_async_copy(buf.at[:, sent, :], buf.at[:, sent, :], sem.at[0]).wait()
    sent = pl.ds(0, depth * rows)
    pltpu.make_async_copy(buf.at[:, sent, :], buf.at[:, sent, :], pair_send.at[0]).wait()
    pltpu.make_async_copy(landed, landed, term_send.at[0]).wait()


def local(devices, pair_elements, gmap, w_screened, coulomb):
    rows, pairs = pair_elements.shape
    elements = pair_elements.at[gmap % rows].get(mode="promise_in_bounds")
    width = pairs // TILES
    depth = devices // 2
    vmem = pl.BlockSpec(memory_space=pltpu.VMEM)
    hbm = pl.BlockSpec(memory_space=pl.ANY)
    screened, sigma = pl.pallas_call(
        functools.partial(kernel, devices),
        out_shape=(
            jax.ShapeDtypeStruct((rows, pairs), jnp.float32),
            jax.ShapeDtypeStruct((1, pairs // devices), jnp.float32),
        ),
        in_specs=[hbm, hbm, vmem],
        out_specs=(vmem, vmem),
        scratch_shapes=[
            pltpu.VMEM((TILES, devices * rows, width), jnp.float32),
            pltpu.VMEM((2, 2 * rows, rows), jnp.float32),
            pltpu.VMEM((rows, 2 * rows), jnp.bfloat16),
            pltpu.VMEM((rows, 2 * rows), jnp.bfloat16),
            pltpu.VMEM((TILES, 1, width), jnp.float32),
            pltpu.VMEM((pairs // 128, 1, 128), jnp.float32),
            pltpu.VMEM((devices - 1, 1, 128), jnp.float32),
            pltpu.SemaphoreType.DMA((depth, TILES)),
            pltpu.SemaphoreType.DMA((depth, TILES)),
            pltpu.SemaphoreType.DMA((1,)),
            pltpu.SemaphoreType.DMA((1,)),
            pltpu.SemaphoreType.DMA((1,)),
            pltpu.SemaphoreType.DMA((TILES,)),
            pltpu.SemaphoreType.DMA((2,)),
            pltpu.SemaphoreType.DMA((1,)),
            pltpu.SemaphoreType.DMA((1,)),
        ],
        compiler_params=pltpu.CompilerParams(
            collective_id=0, has_side_effects=True, vmem_limit_bytes=63 * 1024 * 1024
        ),
        name="ring_screen",
    )(elements, w_screened, coulomb[None, :])
    return screened, sigma.reshape(pairs // devices)


def solution(mesh):
    in_specs = (
        P(("groups", "blk"), None),
        P(("groups", "blk")),
        P("groups", "blk"),
        P(("groups", "blk")),
    )
    out_specs = (P(("groups", "blk"), None), P(("groups", "blk")))
    body = functools.partial(local, mesh.shape["blk"])
    return jax.shard_map(body, mesh=mesh, in_specs=in_specs, out_specs=out_specs, check_vma=False)
```

```python
import functools

import jax
import jax.numpy as jnp
from jax import lax
from jax.experimental import pallas as pl
from jax.experimental.pallas import tpu as pltpu
from jax.sharding import PartitionSpec as P

NB = 64
OCC = 4
TILES = 4
MESH = pl.DeviceIdType.MESH


def split(x):
    hi = x.astype(jnp.bfloat16)
    return hi, (x - hi.astype(jnp.float32)).astype(jnp.bfloat16)


def dot(a, b):
    return jnp.dot(a, b, preferred_element_type=jnp.float32)


def kernel(
    devices,
    e_ref, gmap_ref, w_ref, v_ref, out_ref, sig_ref,
    buf, wbuf, wt_hi, wt_lo, bare, twice, terms, landed,
    ring_recv, pair_recv, right_send, left_send, pair_send, local_sem, w_sem, term_send, term_recv,
):
    rows, pairs = e_ref.shape
    width = pairs // TILES
    depth = devices // 2
    half = depth // 2
    group, me = lax.axis_index("groups"), lax.axis_index("blk")
    z, core = me // 2, me % 2

    def at(blk):
        return (group, blk)

    right = at(lax.rem(z + 1, depth) * 2 + core)
    left = at(lax.rem(z + depth - 1, depth) * 2 + core)
    partner = at(z * 2 + 1 - core)

    barrier = pltpu.get_barrier_semaphore()
    for other in (right, left, partner):
        pl.semaphore_signal(barrier, inc=1, device_id=other, device_id_type=MESH)

    def w_copy(slot, block):
        source = pl.ds(pl.multiple_of(block * 2 * rows, 2 * rows), 2 * rows)
        return pltpu.make_async_copy(w_ref.at[source, :], wbuf.at[slot], w_sem.at[slot])

    def behind(s):
        return lax.rem(z + depth - s, depth)

    def ahead(s):
        return lax.rem(z + s, depth)

    def rows_of(blk):
        return pl.ds(pl.multiple_of(blk * rows, rows), rows)

    def piece(source, which, k):
        return buf.at[k, rows_of(source * 2 + which), :]

    def ring_copy(source, k, send_sem, device):
        return pltpu.make_async_remote_copy(
            src_ref=piece(source, core, k), dst_ref=piece(source, core, k), send_sem=send_sem.at[0],
            recv_sem=ring_recv.at[source, k], device_id=device, device_id_type=MESH)

    def pair_copy(source, which, k):
        return pltpu.make_async_remote_copy(
            src_ref=piece(source, which, k), dst_ref=piece(source, which, k), send_sem=pair_send.at[0],
            recv_sem=pair_recv.at[source, k], device_id=partner, device_id_type=MESH)

    def go_right(source, k):
        ring_copy(source, k, right_send, right).start()

    def go_left(source, k):
        ring_copy(source, k, left_send, left).start()

    def across(source, k):
        pair_copy(source, core, k).start()

    def from_left(source, k):
        ring_copy(source, k, right_send, right).wait_recv()

    def from_right(source, k):
        ring_copy(source, k, left_send, left).wait_recv()

    def take_pair(source, k):
        pair_copy(source, 1 - core, k).wait_recv()

    for k in (0, 3, 1, 2):
        cols = pl.ds(k * width, width)
        pltpu.make_async_copy(e_ref.at[:, cols], out_ref.at[:, cols], local_sem.at[k]).start()
    w_copy(0, z).start()
    w_copy(1, behind(1)).start()
    order = gmap_ref[...].reshape(1, rows) - me * rows
    chosen = (lax.broadcasted_iota(jnp.int32, (rows, rows), 0) == order).astype(jnp.float32)
    chosen = jnp.transpose(chosen).astype(jnp.bfloat16)

    def gather(k):
        cols = slice(k * width, (k + 1) * width)
        pltpu.make_async_copy(e_ref.at[:, cols], out_ref.at[:, cols], local_sem.at[k]).wait()
        raw = out_ref[:, cols]
        hi, rest = raw.astype(jnp.bfloat16), None
        rest = raw - hi.astype(jnp.float32)
        mid, low = split(rest)
        buf[k, rows_of(me), :] = (dot(chosen, hi) + dot(chosen, mid)) + dot(chosen, low)

    gather(0)
    gather(3)
    pl.semaphore_wait(barrier, 3)
    go_right(z, 0)
    go_left(z, 3)
    gather(1)
    gather(2)
    go_right(z, 1)
    go_left(z, 2)
    go_right(z, 2)
    go_left(z, 1)
    go_right(z, 3)
    go_left(z, 0)
    for k in range(TILES):
        across(z, k)

    def load_w(slot, block, to):
        w_copy(slot, block).wait()
        for part in range(2):
            cols = slice(part * rows, part * rows + rows)
            hi, lo = split(jnp.transpose(wbuf[slot, cols, :]))
            wt_hi[to, :, cols] = hi
            wt_lo[to, :, cols] = lo

    def product(k, block, w):
        start = pl.multiple_of(block * 2 * rows, 2 * rows)
        hi, lo = split(buf[k, pl.ds(start, 2 * rows), :])
        return dot(wt_hi[w], hi) + (dot(wt_hi[w], lo) + dot(wt_lo[w], hi))

    def own(k):
        return buf[k, rows_of(me), :]

    def tile(k):
        return pl.ds(pl.multiple_of(k * width, width), width)

    def add_block(block, w):
        def body(k, carry):
            out_ref[:, tile(k)] += product(k, block, w)
            return carry

        lax.fori_loop(0, TILES, body, 0)

    load_w(0, z, 0)
    w_copy(0, ahead(1)).start()
    for k in range(TILES):
        take_pair(z, k)

    def first(k, carry):
        out_ref[:, tile(k)] = product(k, z, 0)
        mine = own(k)
        bare[k] = jnp.dot(v_ref[...].reshape(1, rows), mine * mine, precision=lax.Precision.HIGHEST, preferred_element_type=jnp.float32)
        return carry

    lax.fori_loop(0, TILES, first, 0)

    def step(s, carry):
        for i in range(TILES):
            k = TILES - 1 - i
            from_left(behind(s), i)
            go_right(behind(s), i)
            across(behind(s), i)
            from_right(ahead(s), k)
            go_left(ahead(s), k)
            across(ahead(s), k)
        load_w(1, behind(s), 1)
        w_copy(1, behind(s + 1)).start()
        for k in range(TILES):
            take_pair(behind(s), k)
        add_block(behind(s), 1)
        load_w(0, ahead(s), 0)
        w_copy(0, ahead(s + 1)).start()
        for k in range(TILES):
            take_pair(ahead(s), k)
        add_block(ahead(s), 0)
        return carry

    lax.fori_loop(1, half - 2, step, 0)

    b6, a6, b7, a7, far = behind(half - 2), ahead(half - 2), behind(half - 1), ahead(half - 1), behind(half)
    for i in range(TILES):
        k = TILES - 1 - i
        from_left(b6, i)
        if i < 2:
            go_right(b6, i)
        across(b6, i)
        from_right(a6, k)
        if i < 2:
            go_left(a6, k)
        across(a6, k)
    load_w(1, b6, 1)
    w_copy(1, b7).start()
    for k in range(TILES):
        take_pair(b6, k)
    add_block(b6, 1)

    from_left(b7, 0)
    go_right(b7, 0)
    go_right(b6, 2)
    across(b7, 0)
    from_right(a7, 3)
    go_left(a7, 3)
    go_left(a6, 1)
    across(a7, 3)
    load_w(0, a6, 0)
    w_copy(0, a7).start()
    for k in range(TILES):
        take_pair(a6, k)
    add_block(a6, 0)

    from_left(b7, 1)
    go_right(b7, 1)
    go_right(b6, 3)
    across(b7, 1)
    from_right(a7, 2)
    go_left(a7, 2)
    go_left(a6, 0)
    across(a7, 2)
    load_w(1, b7, 1)
    w_copy(1, far).start()
    load_w(0, a7, 0)
    load_w(1, far, 2)

    def add(k, block, w):
        take_pair(block, k)
        cols = slice(k * width, (k + 1) * width)
        value = product(k, block, w)
        out_ref[:, cols] += value
        return value

    twice[0] = jnp.sum(add(0, b7, 1) * own(0), axis=0, keepdims=True)
    twice[1] = jnp.sum(add(3, a7, 0) * own(3), axis=0, keepdims=True)
    add(1, b7, 1)
    add(2, a7, 0)

    def arrive(source_left, k_left, source_right, k_right):
        from_left(source_left, k_left)
        across(source_left, k_left)
        from_right(source_right, k_right)
        across(source_right, k_right)

    arrive(far, 0, far, 3)
    add(0, far, 2)
    add(3, far, 2)
    arrive(b7, 2, a7, 1)
    add(2, b7, 1)
    add(1, a7, 0)
    arrive(far, 1, far, 2)
    add(1, far, 2)
    add(2, far, 2)

    lanes = terms.shape[-1]
    per_owner = pairs // devices
    owners_per_row = lanes // per_owner
    for k in range(TILES):
        total = jnp.sum(out_ref[:, k * width : (k + 1) * width] * own(k), axis=0, keepdims=True)
        if k == 0:
            total = total + twice[0]
        if k == 3:
            total = total + twice[1]
        pair = lax.broadcasted_iota(jnp.int32, (1, width), 1) + k * width
        coef = jnp.where(pair % NB < OCC, -0.5, 0.5).astype(jnp.float32)
        term = coef * total - 0.5 * bare[k]
        for r in range(width // lanes):
            terms[k * width // lanes + r] = term[:, r * lanes : (r + 1) * lanes]

    def term_copy(owner, slot):
        return pltpu.make_async_remote_copy(
            src_ref=terms.at[owner // owners_per_row], dst_ref=landed.at[slot], send_sem=term_send.at[0],
            recv_sem=term_recv.at[0], device_id=at(owner), device_id_type=MESH)

    def send_term(n, carry):
        owner = lax.rem(me + n, devices)
        term_copy(owner, lax.rem(me - owner - 1 + devices, devices)).start()
        return carry

    lax.fori_loop(1, devices, send_term, 0)

    arrive(b7, 3, a7, 0)
    add(3, b7, 1)
    add(0, a7, 0)

    pltpu.make_async_copy(landed, landed, term_recv.at[0]).wait()
    total = terms[me // owners_per_row] + jnp.sum(landed[...], axis=0)
    place = me % owners_per_row
    mine = total[:, :per_owner]
    for r in range(1, owners_per_row):
        mine = jnp.where(place == r, total[:, r * per_owner : (r + 1) * per_owner], mine)
    sig_ref[...] = mine

    sent = pl.ds(0, (half - 1) * rows + rows // 2)
    for sem in (right_send, left_send):
        pltpu.make_async_copy(buf.at[:, sent, :], buf.at[:, sent, :], sem.at[0]).wait()
    sent = pl.ds(0, depth * rows)
    pltpu.make_async_copy(buf.at[:, sent, :], buf.at[:, sent, :], pair_send.at[0]).wait()
    pltpu.make_async_copy(landed, landed, term_send.at[0]).wait()


def local(devices, pair_elements, gmap, w_screened, coulomb):
    rows, pairs = pair_elements.shape
    width = pairs // TILES
    depth = devices // 2
    vmem = pl.BlockSpec(memory_space=pltpu.VMEM)
    hbm = pl.BlockSpec(memory_space=pl.ANY)
    screened, sigma = pl.pallas_call(
        functools.partial(kernel, devices),
        out_shape=(
            jax.ShapeDtypeStruct((rows, pairs), jnp.float32),
            jax.ShapeDtypeStruct((1, pairs // devices), jnp.float32),
        ),
        in_specs=[hbm, vmem, hbm, vmem],
        out_specs=(vmem, vmem),
        scratch_shapes=[
            pltpu.VMEM((TILES, devices * rows, width), jnp.float32),
            pltpu.VMEM((2, 2 * rows, rows), jnp.float32),
            pltpu.VMEM((3, rows, 2 * rows), jnp.bfloat16),
            pltpu.VMEM((3, rows, 2 * rows), jnp.bfloat16),
            pltpu.VMEM((TILES, 1, width), jnp.float32),
            pltpu.VMEM((2, 1, width), jnp.float32),
            pltpu.VMEM((pairs // 128, 1, 128), jnp.float32),
            pltpu.VMEM((devices - 1, 1, 128), jnp.float32),
            pltpu.SemaphoreType.DMA((depth, TILES)),
            pltpu.SemaphoreType.DMA((depth, TILES)),
            pltpu.SemaphoreType.DMA((1,)),
            pltpu.SemaphoreType.DMA((1,)),
            pltpu.SemaphoreType.DMA((1,)),
            pltpu.SemaphoreType.DMA((TILES,)),
            pltpu.SemaphoreType.DMA((2,)),
            pltpu.SemaphoreType.DMA((1,)),
            pltpu.SemaphoreType.DMA((1,)),
        ],
        compiler_params=pltpu.CompilerParams(
            collective_id=0, has_side_effects=True, vmem_limit_bytes=63 * 1024 * 1024
        ),
        name="ring_screen",
    )(pair_elements, gmap, w_screened, coulomb)
    return screened, sigma.reshape(pairs // devices)


def solution(mesh):
    in_specs = (
        P(("groups", "blk"), None),
        P(("groups", "blk")),
        P("groups", "blk"),
        P(("groups", "blk")),
    )
    out_specs = (P(("groups", "blk"), None), P(("groups", "blk")))
    body = functools.partial(local, mesh.shape["blk"])
    return jax.shard_map(body, mesh=mesh, in_specs=in_specs, out_specs=out_specs, check_vma=False)
```

```python
import functools

import jax
import jax.numpy as jnp
from jax import lax
from jax.experimental import pallas as pl
from jax.experimental.pallas import tpu as pltpu
from jax.sharding import PartitionSpec as P

NB = 64
OCC = 4
TILES = 4
MESH = pl.DeviceIdType.MESH


def split(x):
    hi = x.astype(jnp.bfloat16)
    return hi, (x - hi.astype(jnp.float32)).astype(jnp.bfloat16)


def dot(a, b):
    return jnp.dot(a, b, preferred_element_type=jnp.float32)


def kernel(
    devices,
    e_ref, gmap_ref, w_ref, v_ref, out_ref, sig_ref,
    buf, wbuf, wt_hi, wt_lo, bare, twice, terms, landed,
    ring_recv, pair_recv, right_send, left_send, pair_send, local_sem, w_sem, term_send, term_recv,
):
    rows, pairs = e_ref.shape
    width = pairs // TILES
    depth = devices // 2
    half = depth // 2
    group, me = lax.axis_index("groups"), lax.axis_index("blk")
    z, core = me // 2, me % 2

    def at(blk):
        return (group, blk)

    right = at(lax.rem(z + 1, depth) * 2 + core)
    left = at(lax.rem(z + depth - 1, depth) * 2 + core)
    partner = at(z * 2 + 1 - core)

    barrier = pltpu.get_barrier_semaphore()
    for other in (right, left, partner):
        pl.semaphore_signal(barrier, inc=1, device_id=other, device_id_type=MESH)

    def w_copy(slot, block):
        source = pl.ds(pl.multiple_of(block * 2 * rows, 2 * rows), 2 * rows)
        return pltpu.make_async_copy(w_ref.at[source, :], wbuf.at[slot], w_sem.at[slot])

    def behind(s):
        return lax.rem(z + depth - s, depth)

    def ahead(s):
        return lax.rem(z + s, depth)

    def rows_of(blk):
        return pl.ds(pl.multiple_of(blk * rows, rows), rows)

    def piece(source, which, k):
        return buf.at[k, rows_of(source * 2 + which), :]

    def ring_copy(source, k, send_sem, device):
        return pltpu.make_async_remote_copy(
            src_ref=piece(source, core, k), dst_ref=piece(source, core, k), send_sem=send_sem.at[0],
            recv_sem=ring_recv.at[source, k], device_id=device, device_id_type=MESH)

    def pair_copy(source, which, k):
        return pltpu.make_async_remote_copy(
            src_ref=piece(source, which, k), dst_ref=piece(source, which, k), send_sem=pair_send.at[0],
            recv_sem=pair_recv.at[source, k], device_id=partner, device_id_type=MESH)

    def go_right(source, k):
        ring_copy(source, k, right_send, right).start()

    def go_left(source, k):
        ring_copy(source, k, left_send, left).start()

    def across(source, k):
        pair_copy(source, core, k).start()

    def from_left(source, k):
        ring_copy(source, k, right_send, right).wait_recv()

    def from_right(source, k):
        ring_copy(source, k, left_send, left).wait_recv()

    def take_pair(source, k):
        pair_copy(source, 1 - core, k).wait_recv()

    for k in (0, 3, 1, 2):
        cols = pl.ds(k * width, width)
        pltpu.make_async_copy(e_ref.at[:, cols], out_ref.at[:, cols], local_sem.at[k]).start()
    w_copy(0, z).start()
    w_copy(1, behind(1)).start()
    order = gmap_ref[...].reshape(1, rows) - me * rows
    down = jnp.transpose(jnp.broadcast_to(order.astype(jnp.float32), (128, rows))).astype(jnp.int32)
    lane = lax.broadcasted_iota(jnp.int32, (rows, 128), 1)
    chosen = jnp.concatenate([(down == lane + at128).astype(jnp.float32) for at128 in range(0, rows, 128)], axis=1)
    chosen = chosen.astype(jnp.bfloat16)

    def gather(k):
        cols = slice(k * width, (k + 1) * width)
        pltpu.make_async_copy(e_ref.at[:, cols], out_ref.at[:, cols], local_sem.at[k]).wait()
        raw = out_ref[:, cols]
        hi, rest = raw.astype(jnp.bfloat16), None
        rest = raw - hi.astype(jnp.float32)
        mid, low = split(rest)
        buf[k, rows_of(me), :] = (dot(chosen, hi) + dot(chosen, mid)) + dot(chosen, low)

    gather(0)
    gather(3)
    pl.semaphore_wait(barrier, 3)
    go_right(z, 0)
    go_left(z, 3)
    gather(1)
    gather(2)
    go_right(z, 1)
    go_left(z, 2)
    go_right(z, 2)
    go_left(z, 1)
    go_right(z, 3)
    go_left(z, 0)
    for k in range(TILES):
        across(z, k)

    def load_w(slot, block, to):
        w_copy(slot, block).wait()
        for part in range(2):
            cols = slice(part * rows, part * rows + rows)
            hi, lo = split(jnp.transpose(wbuf[slot, cols, :]))
            wt_hi[to, :, cols] = hi
            wt_lo[to, :, cols] = lo

    def product(k, block, w):
        start = pl.multiple_of(block * 2 * rows, 2 * rows)
        hi, lo = split(buf[k, pl.ds(start, 2 * rows), :])
        return dot(wt_hi[w], hi) + (dot(wt_hi[w], lo) + dot(wt_lo[w], hi))

    def own(k):
        return buf[k, rows_of(me), :]

    def tile(k):
        return pl.ds(pl.multiple_of(k * width, width), width)

    def add_block(block, w):
        def body(k, carry):
            out_ref[:, tile(k)] += product(k, block, w)
            return carry

        lax.fori_loop(0, TILES, body, 0)

    load_w(0, z, 0)
    w_copy(0, ahead(1)).start()
    for k in range(TILES):
        take_pair(z, k)

    def first(k, carry):
        out_ref[:, tile(k)] = product(k, z, 0)
        mine = own(k)
        bare[k] = jnp.dot(v_ref[...].reshape(1, rows), mine * mine, precision=lax.Precision.HIGHEST, preferred_element_type=jnp.float32)
        return carry

    lax.fori_loop(0, TILES, first, 0)

    def step(s, carry):
        for i in range(TILES):
            k = TILES - 1 - i
            from_left(behind(s), i)
            go_right(behind(s), i)
            across(behind(s), i)
            from_right(ahead(s), k)
            go_left(ahead(s), k)
            across(ahead(s), k)
        load_w(1, behind(s), 1)
        w_copy(1, behind(s + 1)).start()
        for k in range(TILES):
            take_pair(behind(s), k)
        add_block(behind(s), 1)
        load_w(0, ahead(s), 0)
        w_copy(0, ahead(s + 1)).start()
        for k in range(TILES):
            take_pair(ahead(s), k)
        add_block(ahead(s), 0)
        return carry

    lax.fori_loop(1, half - 2, step, 0)

    b6, a6, b7, a7, far = behind(half - 2), ahead(half - 2), behind(half - 1), ahead(half - 1), behind(half)
    before_wrap, after_first = z == depth - 1, z == 1
    for i in range(TILES):
        k = TILES - 1 - i
        from_left(b6, i)
        if i < 3:
            go_right(b6, i)
        across(b6, i)
        from_right(a6, k)
        if i < 3:
            go_left(a6, k)
        across(a6, k)
    load_w(1, b6, 1)
    w_copy(1, b7).start()
    for k in range(TILES):
        take_pair(b6, k)
    add_block(b6, 1)

    from_left(b7, 0)
    go_right(b7, 0)
    across(b7, 0)
    from_right(a7, 3)
    go_left(a7, 3)
    across(a7, 3)
    load_w(0, a6, 0)
    w_copy(0, a7).start()
    for k in range(TILES):
        take_pair(a6, k)
    add_block(a6, 0)

    from_left(b7, 1)

    @pl.when(jnp.logical_not(before_wrap))
    def _():
        go_right(b7, 1)

    go_right(b6, 3)
    across(b7, 1)
    from_right(a7, 2)
    go_left(a7, 2)

    @pl.when(jnp.logical_not(after_first))
    def _():
        go_left(a6, 0)

    across(a7, 2)
    load_w(1, b7, 1)
    w_copy(1, far).start()
    load_w(0, a7, 0)
    load_w(1, far, 2)

    def add(k, block, w):
        take_pair(block, k)
        cols = slice(k * width, (k + 1) * width)
        value = product(k, block, w)
        out_ref[:, cols] += value
        return value

    twice[0] = jnp.sum(add(0, b7, 1) * own(0), axis=0, keepdims=True)
    twice[1] = jnp.sum(add(3, a7, 0) * own(3), axis=0, keepdims=True)
    add(1, b7, 1)
    add(2, a7, 0)

    def arrive(source_left, k_left, source_right, k_right):
        from_left(source_left, k_left)
        across(source_left, k_left)
        from_right(source_right, k_right)
        across(source_right, k_right)

    arrive(b7, 2, a7, 1)

    @pl.when(after_first)
    def _():
        go_left(a7, 1)
        go_left(a6, 0)

    add(2, b7, 1)
    add(1, a7, 0)
    arrive(far, 0, far, 3)
    add(0, far, 2)
    add(3, far, 2)
    arrive(far, 1, far, 2)
    add(1, far, 2)
    add(2, far, 2)

    lanes = terms.shape[-1]
    per_owner = pairs // devices
    owners_per_row = lanes // per_owner
    for k in range(TILES):
        total = jnp.sum(out_ref[:, k * width : (k + 1) * width] * own(k), axis=0, keepdims=True)
        if k == 0:
            total = total + twice[0]
        if k == 3:
            total = total + twice[1]
        pair = lax.broadcasted_iota(jnp.int32, (1, width), 1) + k * width
        coef = jnp.where(pair % NB < OCC, -0.5, 0.5).astype(jnp.float32)
        term = coef * total - 0.5 * bare[k]
        for r in range(width // lanes):
            terms[k * width // lanes + r] = term[:, r * lanes : (r + 1) * lanes]

    def term_copy(owner, slot):
        return pltpu.make_async_remote_copy(
            src_ref=terms.at[owner // owners_per_row], dst_ref=landed.at[slot], send_sem=term_send.at[0],
            recv_sem=term_recv.at[0], device_id=at(owner), device_id_type=MESH)

    def send_term(n, carry):
        owner = lax.rem(me + n, devices)
        term_copy(owner, lax.rem(me - owner - 1 + devices, devices)).start()
        return carry

    lax.fori_loop(1, devices, send_term, 0)

    def add_part(k, block, which, w):
        hi, lo = split(buf[k, rows_of(block * 2 + which), :])
        w_hi, w_lo = wt_hi[w, :, rows_of(which)], wt_lo[w, :, rows_of(which)]
        out_ref[:, k * width : (k + 1) * width] += dot(w_hi, hi) + (dot(w_hi, lo) + dot(w_lo, hi))

    arrive(b7, 3, a7, 0)
    add_part(3, b7, core, 1)
    add_part(0, a7, core, 0)
    take_pair(b7, 3)
    add_part(3, b7, 1 - core, 1)
    take_pair(a7, 0)
    add_part(0, a7, 1 - core, 0)

    pltpu.make_async_copy(landed, landed, term_recv.at[0]).wait()
    total = terms[me // owners_per_row] + jnp.sum(landed[...], axis=0)
    place = me % owners_per_row
    mine = total[:, :per_owner]
    for r in range(1, owners_per_row):
        mine = jnp.where(place == r, total[:, r * per_owner : (r + 1) * per_owner], mine)
    sig_ref[...] = mine

    usual = (half - 1) * rows + rows // 2
    piece_rows = rows // TILES
    for sem, odd, count in ((right_send, before_wrap, usual - piece_rows), (left_send, after_first, usual + piece_rows)):

        @pl.when(odd)
        def _(sem=sem, count=count):
            pltpu.make_async_copy(buf.at[:, pl.ds(0, count), :], buf.at[:, pl.ds(0, count), :], sem.at[0]).wait()

        @pl.when(jnp.logical_not(odd))
        def _(sem=sem):
            pltpu.make_async_copy(buf.at[:, pl.ds(0, usual), :], buf.at[:, pl.ds(0, usual), :], sem.at[0]).wait()

    sent = pl.ds(0, depth * rows)
    pltpu.make_async_copy(buf.at[:, sent, :], buf.at[:, sent, :], pair_send.at[0]).wait()
    pltpu.make_async_copy(landed, landed, term_send.at[0]).wait()


def put_out(screened_ref, sigma_ref, out_ref, sig_ref, sems):
    copies = [
        pltpu.make_async_copy(screened_ref, out_ref, sems.at[0]),
        pltpu.make_async_copy(sigma_ref, sig_ref, sems.at[1]),
    ]
    for copy in copies:
        copy.start()
    for copy in copies:
        copy.wait()


def local(devices, pair_elements, gmap, w_screened, coulomb):
    rows, pairs = pair_elements.shape
    width = pairs // TILES
    depth = devices // 2
    vmem = pl.BlockSpec(memory_space=pltpu.VMEM)
    hbm = pl.BlockSpec(memory_space=pl.ANY)
    screened, sigma = pl.pallas_call(
        functools.partial(kernel, devices),
        out_shape=(
            pltpu.VMEM((rows, pairs), jnp.float32),
            pltpu.VMEM((1, pairs // devices), jnp.float32),
        ),
        in_specs=[hbm, vmem, hbm, vmem],
        out_specs=(vmem, vmem),
        scratch_shapes=[
            pltpu.VMEM((TILES, devices * rows, width), jnp.float32),
            pltpu.VMEM((2, 2 * rows, rows), jnp.float32),
            pltpu.VMEM((3, rows, 2 * rows), jnp.bfloat16),
            pltpu.VMEM((3, rows, 2 * rows), jnp.bfloat16),
            pltpu.VMEM((TILES, 1, width), jnp.float32),
            pltpu.VMEM((2, 1, width), jnp.float32),
            pltpu.VMEM((pairs // 128, 1, 128), jnp.float32),
            pltpu.VMEM((devices - 1, 1, 128), jnp.float32),
            pltpu.SemaphoreType.DMA((depth, TILES)),
            pltpu.SemaphoreType.DMA((depth, TILES)),
            pltpu.SemaphoreType.DMA((1,)),
            pltpu.SemaphoreType.DMA((1,)),
            pltpu.SemaphoreType.DMA((1,)),
            pltpu.SemaphoreType.DMA((TILES,)),
            pltpu.SemaphoreType.DMA((2,)),
            pltpu.SemaphoreType.DMA((1,)),
            pltpu.SemaphoreType.DMA((1,)),
        ],
        compiler_params=pltpu.CompilerParams(
            collective_id=0, has_side_effects=True, vmem_limit_bytes=61 * 1024 * 1024
        ),
        name="ring_screen",
    )(pair_elements, gmap, w_screened, coulomb)
    screened, sigma = pl.pallas_call(
        put_out,
        out_shape=(
            jax.ShapeDtypeStruct((rows, pairs), jnp.float32),
            jax.ShapeDtypeStruct((1, pairs // devices), jnp.float32),
        ),
        in_specs=[vmem, vmem],
        out_specs=(hbm, hbm),
        scratch_shapes=[pltpu.SemaphoreType.DMA((2,))],
        compiler_params=pltpu.CompilerParams(vmem_limit_bytes=1024 * 1024),
        name="put_out",
    )(screened, sigma)
    return screened, sigma.reshape(pairs // devices)


def solution(mesh):
    in_specs = (
        P(("groups", "blk"), None),
        P(("groups", "blk")),
        P("groups", "blk"),
        P(("groups", "blk")),
    )
    out_specs = (P(("groups", "blk"), None), P(("groups", "blk")))
    body = functools.partial(local, mesh.shape["blk"])
    return jax.shard_map(body, mesh=mesh, in_specs=in_specs, out_specs=out_specs, check_vma=False)
```

```python
import functools

import jax
import jax.numpy as jnp
from jax import lax
from jax.experimental import pallas as pl
from jax.experimental.pallas import tpu as pltpu
from jax.sharding import PartitionSpec as P

NB = 64
OCC = 4
TILES = 4
MESH = pl.DeviceIdType.MESH


def split(x):
    hi = x.astype(jnp.bfloat16)
    return hi, (x - hi.astype(jnp.float32)).astype(jnp.bfloat16)


def dot(a, b):
    return jnp.dot(a, b, preferred_element_type=jnp.float32)


def kernel(
    devices,
    e_ref, gmap_ref, w_ref, v_ref, out_ref, sig_ref,
    buf, wbuf, wt_hi, wt_lo, bare, twice, terms, landed,
    ring_recv, pair_recv, right_send, left_send, pair_send, local_sem, w_sem, term_send, term_recv, ready,
):
    rows, pairs = e_ref.shape
    width = pairs // TILES
    depth = devices // 2
    half = depth // 2
    group, me = lax.axis_index("groups"), lax.axis_index("blk")
    z, core = me // 2, me % 2

    def at(blk):
        return (group, blk)

    right = at(lax.rem(z + 1, depth) * 2 + core)
    left = at(lax.rem(z + depth - 1, depth) * 2 + core)
    partner = at(z * 2 + 1 - core)

    first_chip, after_first, opposite, before_wrap = z == 0, z == 1, z == half, z == depth - 1

    barrier = pltpu.get_barrier_semaphore()
    for other in (left, partner):
        pl.semaphore_signal(barrier, inc=1, device_id=other, device_id_type=MESH)

    @pl.when(jnp.logical_not(before_wrap))
    def _():
        pl.semaphore_signal(barrier, inc=1, device_id=right, device_id_type=MESH)


    def w_copy(slot, block):
        source = pl.ds(pl.multiple_of(block * 2 * rows, 2 * rows), 2 * rows)
        return pltpu.make_async_copy(w_ref.at[source, :], wbuf.at[slot], w_sem.at[slot])

    def behind(s):
        return lax.rem(z + depth - s, depth)

    def ahead(s):
        return lax.rem(z + s, depth)

    def rows_of(blk):
        return pl.ds(pl.multiple_of(blk * rows, rows), rows)

    def piece(source, which, k):
        return buf.at[k, rows_of(source * 2 + which), :]

    def ring_copy(source, k, send_sem, device):
        return pltpu.make_async_remote_copy(
            src_ref=piece(source, core, k), dst_ref=piece(source, core, k), send_sem=send_sem.at[0],
            recv_sem=ring_recv.at[source, k], device_id=device, device_id_type=MESH)

    def pair_copy(source, which, k):
        return pltpu.make_async_remote_copy(
            src_ref=piece(source, which, k), dst_ref=piece(source, which, k), send_sem=pair_send.at[0],
            recv_sem=pair_recv.at[source, k], device_id=partner, device_id_type=MESH)

    def go_right(source, k):
        ring_copy(source, k, right_send, right).start()

    def go_left(source, k):
        ring_copy(source, k, left_send, left).start()

    def across(source, k):
        pair_copy(source, core, k).start()

    def from_left(source, k):
        ring_copy(source, k, right_send, right).wait_recv()

    def from_right(source, k):
        ring_copy(source, k, left_send, left).wait_recv()

    def take_pair(source, k):
        pair_copy(source, 1 - core, k).wait_recv()

    for k in (0, 3, 1, 2):
        cols = pl.ds(k * width, width)
        pltpu.make_async_copy(e_ref.at[:, cols], out_ref.at[:, cols], local_sem.at[k]).start()
    w_copy(0, z).start()
    w_copy(1, behind(1)).start()
    order = gmap_ref[...].reshape(1, rows) - me * rows
    down = jnp.transpose(jnp.broadcast_to(order.astype(jnp.float32), (128, rows))).astype(jnp.int32)
    lane = lax.broadcasted_iota(jnp.int32, (rows, 128), 1)
    chosen = jnp.concatenate([(down == lane + at128).astype(jnp.float32) for at128 in range(0, rows, 128)], axis=1)
    chosen = chosen.astype(jnp.bfloat16)

    def gather(k):
        cols = slice(k * width, (k + 1) * width)
        pltpu.make_async_copy(e_ref.at[:, cols], out_ref.at[:, cols], local_sem.at[k]).wait()
        raw = out_ref[:, cols]
        hi, rest = raw.astype(jnp.bfloat16), None
        rest = raw - hi.astype(jnp.float32)
        mid, low = split(rest)
        buf[k, rows_of(me), :] = (dot(chosen, hi) + dot(chosen, mid)) + dot(chosen, low)

    def left_unless_first(*tiles):
        @pl.when(jnp.logical_not(first_chip))
        def _():
            for k in tiles:
                go_left(z, k)

    gather(0)
    gather(3)
    pl.semaphore_wait(barrier, jnp.where(first_chip, 2, 3))

    @pl.when(before_wrap)
    def _():
        pl.semaphore_signal(ready, inc=1, device_id=right, device_id_type=MESH)

    go_right(z, 0)
    left_unless_first(3)
    gather(1)
    gather(2)
    for k in (1, 2, 3):
        go_right(z, k)
    left_unless_first(2, 1, 0)
    for k in range(TILES):
        across(z, k)

    def load_w(slot, block, to):
        w_copy(slot, block).wait()
        for part in range(2):
            cols = slice(part * rows, part * rows + rows)
            hi, lo = split(jnp.transpose(wbuf[slot, cols, :]))
            wt_hi[to, :, cols] = hi
            wt_lo[to, :, cols] = lo

    def product(k, block, w):
        start = pl.multiple_of(block * 2 * rows, 2 * rows)
        hi, lo = split(buf[k, pl.ds(start, 2 * rows), :])
        return dot(wt_hi[w], hi) + (dot(wt_hi[w], lo) + dot(wt_lo[w], hi))

    def own(k):
        return buf[k, rows_of(me), :]

    def tile(k):
        return pl.ds(pl.multiple_of(k * width, width), width)

    def add_block(block, w):
        def body(k, carry):
            out_ref[:, tile(k)] += product(k, block, w)
            return carry

        lax.fori_loop(0, TILES, body, 0)

    load_w(0, z, 0)
    w_copy(0, ahead(1)).start()
    for k in range(TILES):
        take_pair(z, k)

    def first(k, carry):
        out_ref[:, tile(k)] = product(k, z, 0)
        mine = own(k)
        bare[k] = jnp.dot(v_ref[...].reshape(1, rows), mine * mine, precision=lax.Precision.HIGHEST, preferred_element_type=jnp.float32)
        return carry

    lax.fori_loop(0, TILES, first, 0)

    @pl.when(first_chip)
    def _():
        pl.semaphore_wait(ready, 1)
        for k in (3, 2, 1, 0):
            go_left(z, k)

    def step(s, carry):
        for i in range(TILES):
            k = TILES - 1 - i
            from_left(behind(s), i)
            go_right(behind(s), i)
            across(behind(s), i)
            from_right(ahead(s), k)
            go_left(ahead(s), k)
            across(ahead(s), k)
        load_w(1, behind(s), 1)
        w_copy(1, behind(s + 1)).start()
        for k in range(TILES):
            take_pair(behind(s), k)
        add_block(behind(s), 1)
        load_w(0, ahead(s), 0)
        w_copy(0, ahead(s + 1)).start()
        for k in range(TILES):
            take_pair(ahead(s), k)
        add_block(ahead(s), 0)
        return carry

    lax.fori_loop(1, half - 3, step, 0)

    b5, b6, b7, far = (behind(half - n) for n in (3, 2, 1, 0))
    a5, a6, a7 = (ahead(half - n) for n in (3, 2, 1))
    def add(k, block, w):
        take_pair(block, k)
        cols = slice(k * width, (k + 1) * width)
        value = product(k, block, w)
        out_ref[:, cols] += value
        return value

    def add_part(k, block, which, w):
        hi, lo = split(buf[k, rows_of(block * 2 + which), :])
        w_hi, w_lo = wt_hi[w, :, rows_of(which)], wt_lo[w, :, rows_of(which)]
        out_ref[:, k * width : (k + 1) * width] += dot(w_hi, hi) + (dot(w_hi, lo) + dot(w_lo, hi))

    def share(value, k):
        return jnp.sum(value * own(k), axis=0, keepdims=True)

    def arrive(source_left, k_left, source_right, k_right, onward=False):
        from_left(source_left, k_left)
        if onward:
            go_right(source_left, k_left)
        across(source_left, k_left)
        from_right(source_right, k_right)
        if onward:
            go_left(source_right, k_right)
        across(source_right, k_right)

    for i in range(TILES):
        arrive(b5, i, a5, TILES - 1 - i, onward=i < 3)
    load_w(1, b5, 1)
    w_copy(1, b6).start()
    for k in range(TILES):
        take_pair(b5, k)
    add_block(b5, 1)
    arrive(b6, 0, a6, 3, onward=True)
    load_w(0, a5, 0)
    w_copy(0, a6).start()
    for k in range(TILES):
        take_pair(a5, k)
    add_block(a5, 0)
    arrive(b6, 1, a6, 2, onward=True)
    go_right(b5, 3)
    go_left(a5, 0)
    load_w(1, b6, 1)
    w_copy(1, b7).start()
    load_w(0, a6, 0)
    w_copy(0, a7).start()
    add(0, b6, 1)
    add(3, a6, 0)
    add(1, b6, 1)
    add(2, a6, 0)
    arrive(b6, 2, a6, 1)
    add(2, b6, 1)
    add(1, a6, 0)
    arrive(b7, 0, a7, 3, onward=True)
    load_w(1, b7, 2)
    w_copy(1, far).start()
    load_w(0, a7, 3)
    twice[0] = share(add(0, b7, 2), 0)
    twice[3] = share(add(3, a7, 3), 3)
    from_left(b7, 1)

    @pl.when(jnp.logical_not(before_wrap))
    def _():
        go_right(b7, 1)

    go_right(b6, 2)
    across(b7, 1)
    from_right(a7, 2)
    go_left(a7, 2)
    go_left(a6, 1)
    across(a7, 2)
    load_w(1, far, 4)
    twice[1] = share(add(1, b7, 2), 1)
    twice[2] = share(add(2, a7, 3), 2)
    arrive(b6, 3, a6, 0, onward=True)
    add(3, b6, 1)
    add(0, a6, 0)
    arrive(far, 0, far, 3)
    add(0, far, 4)
    add(3, far, 4)

    @pl.when(jnp.logical_not(first_chip))
    def _():
        from_left(far, 1)
        across(far, 1)

    from_right(far, 2)
    across(far, 2)

    @pl.when(jnp.logical_not(first_chip))
    def _():
        far_share = share(add(1, far, 4), 1)
        twice[1] += jnp.where(opposite, far_share, 0.0)

    add(2, far, 4)

    lanes = terms.shape[-1]
    per_owner = pairs // devices
    owners_per_row = lanes // per_owner
    for k in range(TILES):
        total = share(out_ref[:, k * width : (k + 1) * width], k) + twice[k]
        pair = lax.broadcasted_iota(jnp.int32, (1, width), 1) + k * width
        coef = jnp.where(pair % NB < OCC, -0.5, 0.5).astype(jnp.float32)
        term = coef * total - 0.5 * bare[k]
        for r in range(width // lanes):
            terms[k * width // lanes + r] = term[:, r * lanes : (r + 1) * lanes]

    def term_copy(owner, slot):
        return pltpu.make_async_remote_copy(
            src_ref=terms.at[owner // owners_per_row], dst_ref=landed.at[slot], send_sem=term_send.at[0],
            recv_sem=term_recv.at[0], device_id=at(owner), device_id_type=MESH)

    def send_term(n, carry):
        owner = lax.rem(me + n, devices)
        term_copy(owner, lax.rem(me - owner - 1 + devices, devices)).start()
        return carry

    lax.fori_loop(1, devices, send_term, 0)

    arrive(b7, 2, a7, 1)

    @pl.when(after_first)
    def _():
        go_left(a7, 1)

    add(2, b7, 2)
    add(1, a7, 3)
    arrive(b7, 3, a7, 0)
    add_part(3, b7, core, 2)
    add_part(0, a7, core, 3)
    take_pair(b7, 3)
    add_part(3, b7, 1 - core, 2)
    take_pair(a7, 0)
    add_part(0, a7, 1 - core, 3)

    @pl.when(first_chip)
    def _():
        from_right(far, 1)
        across(far, 1)
        add_part(1, far, core, 4)
        take_pair(far, 1)
        add_part(1, far, 1 - core, 4)

    pltpu.make_async_copy(landed, landed, term_recv.at[0]).wait()
    total = terms[me // owners_per_row] + jnp.sum(landed[...], axis=0)
    place = me % owners_per_row
    mine = total[:, :per_owner]
    for r in range(1, owners_per_row):
        mine = jnp.where(place == r, total[:, r * per_owner : (r + 1) * per_owner], mine)
    sig_ref[...] = mine

    usual = (half - 1) * rows + rows // 2
    piece_rows = rows // TILES
    for sem, odd, count in ((right_send, before_wrap, usual - piece_rows), (left_send, after_first, usual + piece_rows)):

        @pl.when(odd)
        def _(sem=sem, count=count):
            pltpu.make_async_copy(buf.at[:, pl.ds(0, count), :], buf.at[:, pl.ds(0, count), :], sem.at[0]).wait()

        @pl.when(jnp.logical_not(odd))
        def _(sem=sem):
            pltpu.make_async_copy(buf.at[:, pl.ds(0, usual), :], buf.at[:, pl.ds(0, usual), :], sem.at[0]).wait()

    sent = pl.ds(0, depth * rows)
    pltpu.make_async_copy(buf.at[:, sent, :], buf.at[:, sent, :], pair_send.at[0]).wait()
    pltpu.make_async_copy(landed, landed, term_send.at[0]).wait()


def put_out(screened_ref, sigma_ref, out_ref, sig_ref, sems):
    copies = [
        pltpu.make_async_copy(screened_ref, out_ref, sems.at[0]),
        pltpu.make_async_copy(sigma_ref, sig_ref, sems.at[1]),
    ]
    for copy in copies:
        copy.start()
    for copy in copies:
        copy.wait()


def local(devices, pair_elements, gmap, w_screened, coulomb):
    rows, pairs = pair_elements.shape
    width = pairs // TILES
    depth = devices // 2
    vmem = pl.BlockSpec(memory_space=pltpu.VMEM)
    hbm = pl.BlockSpec(memory_space=pl.ANY)
    screened, sigma = pl.pallas_call(
        functools.partial(kernel, devices),
        out_shape=(
            pltpu.VMEM((rows, pairs), jnp.float32),
            pltpu.VMEM((1, pairs // devices), jnp.float32),
        ),
        in_specs=[hbm, vmem, hbm, vmem],
        out_specs=(vmem, vmem),
        scratch_shapes=[
            pltpu.VMEM((TILES, devices * rows, width), jnp.float32),
            pltpu.VMEM((2, 2 * rows, rows), jnp.float32),
            pltpu.VMEM((5, rows, 2 * rows), jnp.bfloat16),
            pltpu.VMEM((5, rows, 2 * rows), jnp.bfloat16),
            pltpu.VMEM((TILES, 1, width), jnp.float32),
            pltpu.VMEM((TILES, 1, width), jnp.float32),
            pltpu.VMEM((pairs // 128, 1, 128), jnp.float32),
            pltpu.VMEM((devices - 1, 1, 128), jnp.float32),
            pltpu.SemaphoreType.DMA((depth, TILES)),
            pltpu.SemaphoreType.DMA((depth, TILES)),
            pltpu.SemaphoreType.DMA((1,)),
            pltpu.SemaphoreType.DMA((1,)),
            pltpu.SemaphoreType.DMA((1,)),
            pltpu.SemaphoreType.DMA((TILES,)),
            pltpu.SemaphoreType.DMA((2,)),
            pltpu.SemaphoreType.DMA((1,)),
            pltpu.SemaphoreType.DMA((1,)),
            pltpu.SemaphoreType.REGULAR,
        ],
        compiler_params=pltpu.CompilerParams(
            collective_id=0, has_side_effects=True, vmem_limit_bytes=61 * 1024 * 1024
        ),
        name="ring_screen",
    )(pair_elements, gmap, w_screened, coulomb)
    screened, sigma = pl.pallas_call(
        put_out,
        out_shape=(
            jax.ShapeDtypeStruct((rows, pairs), jnp.float32),
            jax.ShapeDtypeStruct((1, pairs // devices), jnp.float32),
        ),
        in_specs=[vmem, vmem],
        out_specs=(hbm, hbm),
        scratch_shapes=[pltpu.SemaphoreType.DMA((2,))],
        compiler_params=pltpu.CompilerParams(vmem_limit_bytes=1024 * 1024),
        name="put_out",
    )(screened, sigma)
    return screened, sigma.reshape(pairs // devices)


def solution(mesh):
    in_specs = (
        P(("groups", "blk"), None),
        P(("groups", "blk")),
        P("groups", "blk"),
        P(("groups", "blk")),
    )
    out_specs = (P(("groups", "blk"), None), P(("groups", "blk")))
    body = functools.partial(local, mesh.shape["blk"])
    return jax.shard_map(body, mesh=mesh, in_specs=in_specs, out_specs=out_specs, check_vma=False)
```

```python
import functools

import jax
import jax.numpy as jnp
from jax import lax
from jax.experimental import pallas as pl
from jax.experimental.pallas import tpu as pltpu
from jax.sharding import PartitionSpec as P

NB = 64
OCC = 4
TILES = 4
MESH = pl.DeviceIdType.MESH


def split(x):
    hi = x.astype(jnp.bfloat16)
    return hi, (x - hi.astype(jnp.float32)).astype(jnp.bfloat16)


def dot(a, b):
    return jnp.dot(a, b, preferred_element_type=jnp.float32)


def kernel(
    devices,
    e_ref, gmap_ref, w_ref, v_ref, out_ref, sig_ref,
    buf, wbuf, wt_hi, wt_lo, bare, twice, terms, landed,
    ring_recv, pair_recv, right_send, left_send, pair_send, local_sem, w_sem, term_send, term_recv, ready, cut_recv,
):
    rows, pairs = e_ref.shape
    width = pairs // TILES
    depth = devices // 2
    half = depth // 2
    group, me = lax.axis_index("groups"), lax.axis_index("blk")
    z, core = me // 2, me % 2

    def at(blk):
        return (group, blk)

    right = at(lax.rem(z + 1, depth) * 2 + core)
    left = at(lax.rem(z + depth - 1, depth) * 2 + core)
    partner = at(z * 2 + 1 - core)

    first_chip, after_first, opposite_first = z == 0, z == 1, z == half
    before_wrap, before_last, opposite_last = z == depth - 1, z == depth - 2, z == half - 1

    barrier = pltpu.get_barrier_semaphore()
    for other in (left, partner):
        pl.semaphore_signal(barrier, inc=1, device_id=other, device_id_type=MESH)

    @pl.when(jnp.logical_not(before_wrap))
    def _():
        pl.semaphore_signal(barrier, inc=1, device_id=right, device_id_type=MESH)


    def w_copy(slot, block):
        source = pl.ds(pl.multiple_of(block * 2 * rows, 2 * rows), 2 * rows)
        return pltpu.make_async_copy(w_ref.at[source, :], wbuf.at[slot], w_sem.at[slot])

    def behind(s):
        return lax.rem(z + depth - s, depth)

    def ahead(s):
        return lax.rem(z + s, depth)

    def rows_of(blk):
        return pl.ds(pl.multiple_of(blk * rows, rows), rows)

    def piece(source, which, k):
        return buf.at[k, rows_of(source * 2 + which), :]

    def ring_copy(source, k, send_sem, device):
        return pltpu.make_async_remote_copy(
            src_ref=piece(source, core, k), dst_ref=piece(source, core, k), send_sem=send_sem.at[0],
            recv_sem=ring_recv.at[source, k], device_id=device, device_id_type=MESH)

    def pair_copy(source, which, k):
        return pltpu.make_async_remote_copy(
            src_ref=piece(source, which, k), dst_ref=piece(source, which, k), send_sem=pair_send.at[0],
            recv_sem=pair_recv.at[source, k], device_id=partner, device_id_type=MESH)

    quarter = rows // 4

    def cut_rows(source, which, k, over):
        start = (source * 2 + which) * rows + (0 if over else quarter)
        return buf.at[k, pl.ds(pl.multiple_of(start, 8), quarter if over else rows - quarter), :]

    def cut_copy(source, k, over, send_sem, device):
        return pltpu.make_async_remote_copy(
            src_ref=cut_rows(source, core, k, over), dst_ref=cut_rows(source, core, k, over), send_sem=send_sem.at[0],
            recv_sem=cut_recv.at[0 if over else 1], device_id=device, device_id_type=MESH)

    def cut_pair(source, which, k, over):
        return pltpu.make_async_remote_copy(
            src_ref=cut_rows(source, which, k, over), dst_ref=cut_rows(source, which, k, over), send_sem=pair_send.at[0],
            recv_sem=cut_recv.at[2 if over else 3], device_id=partner, device_id_type=MESH)

    def go_right(source, k):
        ring_copy(source, k, right_send, right).start()

    def go_left(source, k):
        ring_copy(source, k, left_send, left).start()

    def across(source, k):
        pair_copy(source, core, k).start()

    def from_left(source, k):
        ring_copy(source, k, right_send, right).wait_recv()

    def from_right(source, k):
        ring_copy(source, k, left_send, left).wait_recv()

    def take_pair(source, k):
        pair_copy(source, 1 - core, k).wait_recv()

    for k in (0, 3, 1, 2):
        cols = pl.ds(k * width, width)
        pltpu.make_async_copy(e_ref.at[:, cols], out_ref.at[:, cols], local_sem.at[k]).start()
    w_copy(0, z).start()
    w_copy(1, behind(1)).start()
    order = gmap_ref[...].reshape(1, rows) - me * rows
    down = jnp.transpose(jnp.broadcast_to(order.astype(jnp.float32), (128, rows))).astype(jnp.int32)
    lane = lax.broadcasted_iota(jnp.int32, (rows, 128), 1)
    chosen = jnp.concatenate([(down == lane + at128).astype(jnp.float32) for at128 in range(0, rows, 128)], axis=1)
    chosen = chosen.astype(jnp.bfloat16)

    def gather(k):
        cols = slice(k * width, (k + 1) * width)
        pltpu.make_async_copy(e_ref.at[:, cols], out_ref.at[:, cols], local_sem.at[k]).wait()
        raw = out_ref[:, cols]
        hi, rest = raw.astype(jnp.bfloat16), None
        rest = raw - hi.astype(jnp.float32)
        mid, low = split(rest)
        buf[k, rows_of(me), :] = (dot(chosen, hi) + dot(chosen, mid)) + dot(chosen, low)

    def left_unless_first(*tiles):
        @pl.when(jnp.logical_not(first_chip))
        def _():
            for k in tiles:
                go_left(z, k)

    gather(0)
    gather(3)
    pl.semaphore_wait(barrier, jnp.where(first_chip, 2, 3))

    @pl.when(before_wrap)
    def _():
        pl.semaphore_signal(ready, inc=1, device_id=right, device_id_type=MESH)

    go_right(z, 0)
    left_unless_first(3)
    gather(1)
    gather(2)
    for k in (1, 2, 3):
        go_right(z, k)
    left_unless_first(2, 1, 0)
    for k in range(TILES):
        across(z, k)

    def load_w(slot, block, to):
        w_copy(slot, block).wait()
        for part in range(2):
            cols = slice(part * rows, part * rows + rows)
            hi, lo = split(jnp.transpose(wbuf[slot, cols, :]))
            wt_hi[to, :, cols] = hi
            wt_lo[to, :, cols] = lo

    def product(k, block, w):
        start = pl.multiple_of(block * 2 * rows, 2 * rows)
        hi, lo = split(buf[k, pl.ds(start, 2 * rows), :])
        return dot(wt_hi[w], hi) + (dot(wt_hi[w], lo) + dot(wt_lo[w], hi))

    def own(k):
        return buf[k, rows_of(me), :]

    def tile(k):
        return pl.ds(pl.multiple_of(k * width, width), width)

    def add_block(block, w):
        def body(k, carry):
            out_ref[:, tile(k)] += product(k, block, w)
            return carry

        lax.fori_loop(0, TILES, body, 0)

    load_w(0, z, 0)
    w_copy(0, ahead(1)).start()
    for k in range(TILES):
        take_pair(z, k)

    def first(k, carry):
        out_ref[:, tile(k)] = product(k, z, 0)
        mine = own(k)
        bare[k] = jnp.dot(v_ref[...].reshape(1, rows), mine * mine, precision=lax.Precision.HIGHEST, preferred_element_type=jnp.float32)
        return carry

    lax.fori_loop(0, TILES, first, 0)

    @pl.when(first_chip)
    def _():
        pl.semaphore_wait(ready, 1)
        for k in (3, 2, 1, 0):
            go_left(z, k)

    def step(s, carry):
        for i in range(TILES):
            k = TILES - 1 - i
            from_left(behind(s), i)
            go_right(behind(s), i)
            across(behind(s), i)
            from_right(ahead(s), k)
            go_left(ahead(s), k)
            across(ahead(s), k)
        load_w(1, behind(s), 1)
        w_copy(1, behind(s + 1)).start()
        for k in range(TILES):
            take_pair(behind(s), k)
        add_block(behind(s), 1)
        load_w(0, ahead(s), 0)
        w_copy(0, ahead(s + 1)).start()
        for k in range(TILES):
            take_pair(ahead(s), k)
        add_block(ahead(s), 0)
        return carry

    lax.fori_loop(1, half - 3, step, 0)

    b5, b6, b7, far = (behind(half - n) for n in (3, 2, 1, 0))
    a5, a6, a7 = (ahead(half - n) for n in (3, 2, 1))
    def add(k, block, w):
        take_pair(block, k)
        cols = slice(k * width, (k + 1) * width)
        value = product(k, block, w)
        out_ref[:, cols] += value
        return value

    def add_part(k, block, which, w):
        hi, lo = split(buf[k, rows_of(block * 2 + which), :])
        w_hi, w_lo = wt_hi[w, :, rows_of(which)], wt_lo[w, :, rows_of(which)]
        out_ref[:, k * width : (k + 1) * width] += dot(w_hi, hi) + (dot(w_hi, lo) + dot(w_lo, hi))

    def share(value, k):
        return jnp.sum(value * own(k), axis=0, keepdims=True)

    def arrive(source_left, k_left, source_right, k_right, onward=False):
        from_left(source_left, k_left)
        if onward:
            go_right(source_left, k_left)
        across(source_left, k_left)
        from_right(source_right, k_right)
        if onward:
            go_left(source_right, k_right)
        across(source_right, k_right)

    for i in range(TILES):
        arrive(b5, i, a5, TILES - 1 - i, onward=i < 3)
    load_w(1, b5, 1)
    w_copy(1, b6).start()
    for k in range(TILES):
        take_pair(b5, k)
    add_block(b5, 1)
    arrive(b6, 0, a6, 3, onward=True)
    load_w(0, a5, 0)
    w_copy(0, a6).start()
    for k in range(TILES):
        take_pair(a5, k)
    add_block(a5, 0)
    arrive(b6, 1, a6, 2, onward=True)
    go_right(b5, 3)
    go_left(a5, 0)
    load_w(1, b6, 1)
    w_copy(1, b7).start()
    load_w(0, a6, 0)
    w_copy(0, a7).start()
    add(0, b6, 1)
    add(3, a6, 0)
    add(1, b6, 1)
    add(2, a6, 0)
    arrive(b6, 2, a6, 1)
    add(2, b6, 1)
    add(1, a6, 0)
    arrive(b7, 0, a7, 3, onward=True)
    load_w(1, b7, 2)
    w_copy(1, far).start()
    load_w(0, a7, 3)
    twice[0] = share(add(0, b7, 2), 0)
    twice[3] = share(add(3, a7, 3), 3)
    from_left(b7, 1)

    @pl.when(jnp.logical_not(before_wrap))
    def _():
        go_right(b7, 1)

    @pl.when(before_wrap)
    def _():
        cut_copy(b7, 1, True, right_send, right).start()

    go_right(b6, 2)
    across(b7, 1)
    from_right(a7, 2)

    @pl.when(jnp.logical_not(first_chip))
    def _():
        go_left(a7, 2)

    @pl.when(first_chip)
    def _():
        cut_copy(a7, 2, True, left_send, left).start()

    go_left(a6, 1)
    across(a7, 2)
    load_w(1, far, 4)
    twice[1] = share(add(1, b7, 2), 1)
    twice[2] = share(add(2, a7, 3), 2)
    arrive(b6, 3, a6, 0)
    add(3, b6, 1)
    add(0, a6, 0)
    arrive(far, 0, far, 3)
    add(0, far, 4)
    add(3, far, 4)

    @pl.when(jnp.logical_not(first_chip))
    def _():
        from_left(far, 1)
        across(far, 1)

    @pl.when(first_chip)
    def _():
        cut_copy(far, 1, True, right_send, right).wait_recv()
        cut_pair(far, core, 1, True).start()

    @pl.when(jnp.logical_not(before_wrap))
    def _():
        from_right(far, 2)
        across(far, 2)

    @pl.when(before_wrap)
    def _():
        cut_copy(far, 2, True, left_send, left).wait_recv()
        cut_pair(far, core, 2, True).start()

    for k, absent, opposite in ((1, first_chip, opposite_first), (2, before_wrap, opposite_last)):

        @pl.when(jnp.logical_not(absent))
        def _(k=k, opposite=opposite):
            twice[k] += jnp.where(opposite, share(add(k, far, 4), k), 0.0)

    lanes = terms.shape[-1]
    per_owner = pairs // devices
    owners_per_row = lanes // per_owner
    for k in range(TILES):
        total = share(out_ref[:, k * width : (k + 1) * width], k) + twice[k]
        pair = lax.broadcasted_iota(jnp.int32, (1, width), 1) + k * width
        coef = jnp.where(pair % NB < OCC, -0.5, 0.5).astype(jnp.float32)
        term = coef * total - 0.5 * bare[k]
        for r in range(width // lanes):
            terms[k * width // lanes + r] = term[:, r * lanes : (r + 1) * lanes]

    def term_copy(owner, slot):
        return pltpu.make_async_remote_copy(
            src_ref=terms.at[owner // owners_per_row], dst_ref=landed.at[slot], send_sem=term_send.at[0],
            recv_sem=term_recv.at[0], device_id=at(owner), device_id_type=MESH)

    def send_term(n, carry):
        owner = lax.rem(me + n, devices)
        term_copy(owner, lax.rem(me - owner - 1 + devices, devices)).start()
        return carry

    lax.fori_loop(1, devices, send_term, 0)
    go_right(b6, 3)
    go_left(a6, 0)

    arrive(b7, 2, a7, 1)

    @pl.when(before_last)
    def _():
        cut_copy(b7, 2, False, right_send, right).start()

    @pl.when(after_first)
    def _():
        cut_copy(a7, 1, False, left_send, left).start()

    add(2, b7, 2)
    add(1, a7, 3)
    arrive(b7, 3, a7, 0)
    add_part(3, b7, core, 2)
    add_part(0, a7, core, 3)
    take_pair(b7, 3)
    add_part(3, b7, 1 - core, 2)
    take_pair(a7, 0)
    add_part(0, a7, 1 - core, 3)

    for k, absent in ((1, first_chip), (2, before_wrap)):

        @pl.when(absent)
        def _(k=k):
            cut_copy(far, k, False, right_send, right).wait_recv()
            cut_pair(far, core, k, False).start()
            add_part(k, far, core, 4)
            for over in (True, False):
                cut_pair(far, 1 - core, k, over).wait_recv()
            add_part(k, far, 1 - core, 4)

    pltpu.make_async_copy(landed, landed, term_recv.at[0]).wait()
    total = terms[me // owners_per_row] + jnp.sum(landed[...], axis=0)
    place = me % owners_per_row
    mine = total[:, :per_owner]
    for r in range(1, owners_per_row):
        mine = jnp.where(place == r, total[:, r * per_owner : (r + 1) * per_owner], mine)
    sig_ref[...] = mine

    usual = (half - 1) * rows + rows // 2
    cut = (rows - quarter) // TILES
    for sem, less, more in ((right_send, before_wrap, before_last), (left_send, first_chip, after_first)):
        for case, count in (
            (less, usual - cut),
            (more, usual + cut),
            (jnp.logical_not(jnp.logical_or(less, more)), usual),
        ):

            @pl.when(case)
            def _(sem=sem, count=count):
                pltpu.make_async_copy(buf.at[:, pl.ds(0, count), :], buf.at[:, pl.ds(0, count), :], sem.at[0]).wait()

    sent = pl.ds(0, depth * rows)
    pltpu.make_async_copy(buf.at[:, sent, :], buf.at[:, sent, :], pair_send.at[0]).wait()
    pltpu.make_async_copy(landed, landed, term_send.at[0]).wait()


def put_out(screened_ref, sigma_ref, out_ref, sig_ref, sems):
    copies = [
        pltpu.make_async_copy(screened_ref, out_ref, sems.at[0]),
        pltpu.make_async_copy(sigma_ref, sig_ref, sems.at[1]),
    ]
    for copy in copies:
        copy.start()
    for copy in copies:
        copy.wait()


def local(devices, pair_elements, gmap, w_screened, coulomb):
    rows, pairs = pair_elements.shape
    width = pairs // TILES
    depth = devices // 2
    vmem = pl.BlockSpec(memory_space=pltpu.VMEM)
    hbm = pl.BlockSpec(memory_space=pl.ANY)
    screened, sigma = pl.pallas_call(
        functools.partial(kernel, devices),
        out_shape=(
            pltpu.VMEM((rows, pairs), jnp.float32),
            pltpu.VMEM((1, pairs // devices), jnp.float32),
        ),
        in_specs=[hbm, vmem, hbm, vmem],
        out_specs=(vmem, vmem),
        scratch_shapes=[
            pltpu.VMEM((TILES, devices * rows, width), jnp.float32),
            pltpu.VMEM((2, 2 * rows, rows), jnp.float32),
            pltpu.VMEM((5, rows, 2 * rows), jnp.bfloat16),
            pltpu.VMEM((5, rows, 2 * rows), jnp.bfloat16),
            pltpu.VMEM((TILES, 1, width), jnp.float32),
            pltpu.VMEM((TILES, 1, width), jnp.float32),
            pltpu.VMEM((pairs // 128, 1, 128), jnp.float32),
            pltpu.VMEM((devices - 1, 1, 128), jnp.float32),
            pltpu.SemaphoreType.DMA((depth, TILES)),
            pltpu.SemaphoreType.DMA((depth, TILES)),
            pltpu.SemaphoreType.DMA((1,)),
            pltpu.SemaphoreType.DMA((1,)),
            pltpu.SemaphoreType.DMA((1,)),
            pltpu.SemaphoreType.DMA((TILES,)),
            pltpu.SemaphoreType.DMA((2,)),
            pltpu.SemaphoreType.DMA((1,)),
            pltpu.SemaphoreType.DMA((1,)),
            pltpu.SemaphoreType.REGULAR,
            pltpu.SemaphoreType.DMA((4,)),
        ],
        compiler_params=pltpu.CompilerParams(
            collective_id=0, has_side_effects=True, vmem_limit_bytes=61 * 1024 * 1024
        ),
        name="ring_screen",
    )(pair_elements, gmap, w_screened, coulomb)
    screened, sigma = pl.pallas_call(
        put_out,
        out_shape=(
            jax.ShapeDtypeStruct((rows, pairs), jnp.float32),
            jax.ShapeDtypeStruct((1, pairs // devices), jnp.float32),
        ),
        in_specs=[vmem, vmem],
        out_specs=(hbm, hbm),
        scratch_shapes=[pltpu.SemaphoreType.DMA((2,))],
        compiler_params=pltpu.CompilerParams(vmem_limit_bytes=1024 * 1024),
        name="put_out",
    )(screened, sigma)
    return screened, sigma.reshape(pairs // devices)


def solution(mesh):
    in_specs = (
        P(("groups", "blk"), None),
        P(("groups", "blk")),
        P("groups", "blk"),
        P(("groups", "blk")),
    )
    out_specs = (P(("groups", "blk"), None), P(("groups", "blk")))
    body = functools.partial(local, mesh.shape["blk"])
    return jax.shard_map(body, mesh=mesh, in_specs=in_specs, out_specs=out_specs, check_vma=False)
```

```python
import functools

import jax
import jax.numpy as jnp
from jax import lax
from jax.experimental import pallas as pl
from jax.experimental.pallas import tpu as pltpu
from jax.sharding import PartitionSpec as P

NB = 64
OCC = 4
TILES = 4
MESH = pl.DeviceIdType.MESH


def split(x):
    hi = x.astype(jnp.bfloat16)
    return hi, (x - hi.astype(jnp.float32)).astype(jnp.bfloat16)


def dot(a, b):
    return jnp.dot(a, b, preferred_element_type=jnp.float32)


def kernel(
    devices,
    e_ref, gmap_ref, w_ref, v_ref, out_ref, sig_ref,
    buf, wbuf, wt_hi, wt_lo, bare, twice, terms, landed,
    ring_recv, pair_recv, right_send, left_send, pair_send, local_sem, w_sem, term_send, term_recv, ready, cut_recv,
):
    rows, pairs = e_ref.shape
    width = pairs // TILES
    depth = devices // 2
    half = depth // 2
    group, me = lax.axis_index("groups"), lax.axis_index("blk")
    z, core = me // 2, me % 2

    def at(blk):
        return (group, blk)

    right = at(lax.rem(z + 1, depth) * 2 + core)
    left = at(lax.rem(z + depth - 1, depth) * 2 + core)
    partner = at(z * 2 + 1 - core)

    first_chip, after_first, opposite_first = z == 0, z == 1, z == half
    before_wrap, before_last, opposite_last = z == depth - 1, z == depth - 2, z == half - 1

    barrier = pltpu.get_barrier_semaphore()
    for other in (left, partner):
        pl.semaphore_signal(barrier, inc=1, device_id=other, device_id_type=MESH)

    @pl.when(jnp.logical_not(before_wrap))
    def _():
        pl.semaphore_signal(barrier, inc=1, device_id=right, device_id_type=MESH)


    def w_copy(slot, block):
        source = pl.ds(pl.multiple_of(block * 2 * rows, 2 * rows), 2 * rows)
        return pltpu.make_async_copy(w_ref.at[source, :], wbuf.at[slot], w_sem.at[slot])

    def behind(s):
        return lax.rem(z + depth - s, depth)

    def ahead(s):
        return lax.rem(z + s, depth)

    def rows_of(blk):
        return pl.ds(pl.multiple_of(blk * rows, rows), rows)

    def piece(source, which, k):
        return buf.at[k, rows_of(source * 2 + which), :]

    def ring_copy(source, k, send_sem, device):
        return pltpu.make_async_remote_copy(
            src_ref=piece(source, core, k), dst_ref=piece(source, core, k), send_sem=send_sem.at[0],
            recv_sem=ring_recv.at[source, k], device_id=device, device_id_type=MESH)

    def pair_copy(source, which, k):
        return pltpu.make_async_remote_copy(
            src_ref=piece(source, which, k), dst_ref=piece(source, which, k), send_sem=pair_send.at[0],
            recv_sem=pair_recv.at[source, k], device_id=partner, device_id_type=MESH)

    quarter = rows // 4

    def cut_rows(source, which, k, over):
        start = (source * 2 + which) * rows + (0 if over else quarter)
        return buf.at[k, pl.ds(pl.multiple_of(start, 8), quarter if over else rows - quarter), :]

    def cut_copy(source, k, over, send_sem, device):
        return pltpu.make_async_remote_copy(
            src_ref=cut_rows(source, core, k, over), dst_ref=cut_rows(source, core, k, over), send_sem=send_sem.at[0],
            recv_sem=cut_recv.at[0 if over else 1], device_id=device, device_id_type=MESH)

    def cut_pair(source, which, k, over):
        return pltpu.make_async_remote_copy(
            src_ref=cut_rows(source, which, k, over), dst_ref=cut_rows(source, which, k, over), send_sem=pair_send.at[0],
            recv_sem=cut_recv.at[2 if over else 3], device_id=partner, device_id_type=MESH)

    def go_right(source, k):
        ring_copy(source, k, right_send, right).start()

    def go_left(source, k):
        ring_copy(source, k, left_send, left).start()

    def across(source, k):
        pair_copy(source, core, k).start()

    def from_left(source, k):
        ring_copy(source, k, right_send, right).wait_recv()

    def from_right(source, k):
        ring_copy(source, k, left_send, left).wait_recv()

    def take_pair(source, k):
        pair_copy(source, 1 - core, k).wait_recv()

    for k in (3, 0, 2, 1):
        cols = pl.ds(k * width, width)
        pltpu.make_async_copy(e_ref.at[:, cols], out_ref.at[:, cols], local_sem.at[k]).start()
    w_copy(0, z).start()
    w_copy(1, behind(1)).start()
    order = gmap_ref[...].reshape(1, rows) - me * rows
    down = jnp.transpose(jnp.broadcast_to(order.astype(jnp.float32), (128, rows))).astype(jnp.int32)
    lane = lax.broadcasted_iota(jnp.int32, (rows, 128), 1)
    chosen = jnp.concatenate([(down == lane + at128).astype(jnp.float32) for at128 in range(0, rows, 128)], axis=1)
    chosen = chosen.astype(jnp.bfloat16)

    def gather(k):
        cols = slice(k * width, (k + 1) * width)
        pltpu.make_async_copy(e_ref.at[:, cols], out_ref.at[:, cols], local_sem.at[k]).wait()
        raw = out_ref[:, cols]
        hi, rest = raw.astype(jnp.bfloat16), None
        rest = raw - hi.astype(jnp.float32)
        mid, low = split(rest)
        buf[k, rows_of(me), :] = (dot(chosen, hi) + dot(chosen, mid)) + dot(chosen, low)

    def left_unless_first(*tiles):
        @pl.when(jnp.logical_not(first_chip))
        def _():
            for k in tiles:
                go_left(z, k)

    @pl.when(before_wrap)
    def _():
        pl.semaphore_wait(barrier, 3)
        pl.semaphore_signal(ready, inc=1, device_id=right, device_id_type=MESH)

    gather(3)

    @pl.when(jnp.logical_not(before_wrap))
    def _():
        pl.semaphore_wait(barrier, jnp.where(first_chip, 2, 3))

    left_unless_first(3)
    gather(0)

    go_right(z, 0)
    gather(1)
    gather(2)
    for k in (1, 2, 3):
        go_right(z, k)
    left_unless_first(2, 1, 0)
    for k in range(TILES):
        across(z, k)

    def load_w(slot, block, to):
        w_copy(slot, block).wait()
        for part in range(2):
            cols = slice(part * rows, part * rows + rows)
            hi, lo = split(jnp.transpose(wbuf[slot, cols, :]))
            wt_hi[to, :, cols] = hi
            wt_lo[to, :, cols] = lo

    def product(k, block, w):
        start = pl.multiple_of(block * 2 * rows, 2 * rows)
        hi, lo = split(buf[k, pl.ds(start, 2 * rows), :])
        return dot(wt_hi[w], hi) + (dot(wt_hi[w], lo) + dot(wt_lo[w], hi))

    def own(k):
        return buf[k, rows_of(me), :]

    def tile(k):
        return pl.ds(pl.multiple_of(k * width, width), width)

    def add_block(block, w):
        def body(k, carry):
            out_ref[:, tile(k)] += product(k, block, w)
            return carry

        lax.fori_loop(0, TILES, body, 0)

    load_w(0, z, 0)
    w_copy(0, ahead(1)).start()
    for k in range(TILES):
        take_pair(z, k)

    def first(k, carry):
        out_ref[:, tile(k)] = product(k, z, 0)
        mine = own(k)
        bare[k] = jnp.dot(v_ref[...].reshape(1, rows), mine * mine, precision=lax.Precision.HIGHEST, preferred_element_type=jnp.float32)
        return carry

    lax.fori_loop(0, TILES, first, 0)

    @pl.when(first_chip)
    def _():
        pl.semaphore_wait(ready, 1)
        for k in (3, 2, 1, 0):
            go_left(z, k)

    def step(s, carry):
        for i in range(TILES):
            k = TILES - 1 - i
            from_left(behind(s), i)
            go_right(behind(s), i)
            across(behind(s), i)
            from_right(ahead(s), k)
            go_left(ahead(s), k)
            across(ahead(s), k)
        load_w(1, behind(s), 1)
        w_copy(1, behind(s + 1)).start()
        for k in range(TILES):
            take_pair(behind(s), k)
        add_block(behind(s), 1)
        load_w(0, ahead(s), 0)
        w_copy(0, ahead(s + 1)).start()
        for k in range(TILES):
            take_pair(ahead(s), k)
        add_block(ahead(s), 0)
        return carry

    lax.fori_loop(1, half - 3, step, 0)

    b5, b6, b7, far = (behind(half - n) for n in (3, 2, 1, 0))
    a5, a6, a7 = (ahead(half - n) for n in (3, 2, 1))
    def add(k, block, w):
        take_pair(block, k)
        cols = slice(k * width, (k + 1) * width)
        value = product(k, block, w)
        out_ref[:, cols] += value
        return value

    def add_part(k, block, which, w):
        hi, lo = split(buf[k, rows_of(block * 2 + which), :])
        w_hi, w_lo = wt_hi[w, :, rows_of(which)], wt_lo[w, :, rows_of(which)]
        out_ref[:, k * width : (k + 1) * width] += dot(w_hi, hi) + (dot(w_hi, lo) + dot(w_lo, hi))

    def share(value, k):
        return jnp.sum(value * own(k), axis=0, keepdims=True)

    def arrive(source_left, k_left, source_right, k_right, onward=False):
        from_left(source_left, k_left)
        if onward:
            go_right(source_left, k_left)
        across(source_left, k_left)
        from_right(source_right, k_right)
        if onward:
            go_left(source_right, k_right)
        across(source_right, k_right)

    for i in range(TILES):
        arrive(b5, i, a5, TILES - 1 - i, onward=i < 3)
    load_w(1, b5, 1)
    w_copy(1, b6).start()
    for k in range(TILES):
        take_pair(b5, k)
    add_block(b5, 1)
    arrive(b6, 0, a6, 3, onward=True)
    load_w(0, a5, 0)
    w_copy(0, a6).start()
    for k in range(TILES):
        take_pair(a5, k)
    add_block(a5, 0)
    arrive(b6, 1, a6, 2, onward=True)
    go_right(b5, 3)
    go_left(a5, 0)
    load_w(1, b6, 1)
    w_copy(1, b7).start()
    load_w(0, a6, 0)
    w_copy(0, a7).start()
    add(0, b6, 1)
    add(3, a6, 0)
    add(1, b6, 1)
    add(2, a6, 0)
    arrive(b6, 2, a6, 1)
    add(2, b6, 1)
    add(1, a6, 0)
    arrive(b7, 0, a7, 3, onward=True)
    load_w(1, b7, 2)
    w_copy(1, far).start()
    load_w(0, a7, 3)
    twice[0] = share(add(0, b7, 2), 0)
    twice[3] = share(add(3, a7, 3), 3)
    from_left(b7, 1)

    @pl.when(jnp.logical_not(before_wrap))
    def _():
        go_right(b7, 1)

    @pl.when(before_wrap)
    def _():
        cut_copy(b7, 1, True, right_send, right).start()

    go_right(b6, 2)
    across(b7, 1)
    from_right(a7, 2)

    @pl.when(jnp.logical_not(first_chip))
    def _():
        go_left(a7, 2)

    @pl.when(first_chip)
    def _():
        cut_copy(a7, 2, True, left_send, left).start()

    go_left(a6, 1)
    across(a7, 2)
    load_w(1, far, 4)
    twice[1] = share(add(1, b7, 2), 1)
    twice[2] = share(add(2, a7, 3), 2)
    arrive(b6, 3, a6, 0)
    add(3, b6, 1)
    add(0, a6, 0)
    arrive(far, 0, far, 3)
    add(0, far, 4)
    add(3, far, 4)

    @pl.when(jnp.logical_not(first_chip))
    def _():
        from_left(far, 1)
        across(far, 1)

    @pl.when(first_chip)
    def _():
        cut_copy(far, 1, True, right_send, right).wait_recv()
        cut_pair(far, core, 1, True).start()

    @pl.when(jnp.logical_not(before_wrap))
    def _():
        from_right(far, 2)
        across(far, 2)

    @pl.when(before_wrap)
    def _():
        cut_copy(far, 2, True, left_send, left).wait_recv()
        cut_pair(far, core, 2, True).start()

    for k, absent, opposite in ((1, first_chip, opposite_first), (2, before_wrap, opposite_last)):

        @pl.when(jnp.logical_not(absent))
        def _(k=k, opposite=opposite):
            twice[k] += jnp.where(opposite, share(add(k, far, 4), k), 0.0)

    lanes = terms.shape[-1]
    per_owner = pairs // devices
    owners_per_row = lanes // per_owner
    for k in range(TILES):
        total = share(out_ref[:, k * width : (k + 1) * width], k) + twice[k]
        pair = lax.broadcasted_iota(jnp.int32, (1, width), 1) + k * width
        coef = jnp.where(pair % NB < OCC, -0.5, 0.5).astype(jnp.float32)
        term = coef * total - 0.5 * bare[k]
        for r in range(width // lanes):
            terms[k * width // lanes + r] = term[:, r * lanes : (r + 1) * lanes]

    def term_copy(owner, slot):
        return pltpu.make_async_remote_copy(
            src_ref=terms.at[owner // owners_per_row], dst_ref=landed.at[slot], send_sem=term_send.at[0],
            recv_sem=term_recv.at[0], device_id=at(owner), device_id_type=MESH)

    def send_term(n, carry):
        owner = lax.rem(me + n, devices)
        term_copy(owner, lax.rem(me - owner - 1 + devices, devices)).start()
        return carry

    lax.fori_loop(1, devices, send_term, 0)
    go_right(b6, 3)
    go_left(a6, 0)

    arrive(b7, 2, a7, 1)

    @pl.when(before_last)
    def _():
        cut_copy(b7, 2, False, right_send, right).start()

    @pl.when(after_first)
    def _():
        cut_copy(a7, 1, False, left_send, left).start()

    add(2, b7, 2)
    add(1, a7, 3)
    arrive(b7, 3, a7, 0)
    add_part(3, b7, core, 2)
    add_part(0, a7, core, 3)
    take_pair(b7, 3)
    add_part(3, b7, 1 - core, 2)
    take_pair(a7, 0)
    add_part(0, a7, 1 - core, 3)

    for k, absent in ((1, first_chip), (2, before_wrap)):

        @pl.when(absent)
        def _(k=k):
            cut_copy(far, k, False, right_send, right).wait_recv()
            cut_pair(far, core, k, False).start()
            add_part(k, far, core, 4)
            for over in (True, False):
                cut_pair(far, 1 - core, k, over).wait_recv()
            add_part(k, far, 1 - core, 4)

    pltpu.make_async_copy(landed, landed, term_recv.at[0]).wait()
    total = terms[me // owners_per_row] + jnp.sum(landed[...], axis=0)
    place = me % owners_per_row
    mine = total[:, :per_owner]
    for r in range(1, owners_per_row):
        mine = jnp.where(place == r, total[:, r * per_owner : (r + 1) * per_owner], mine)
    sig_ref[...] = mine

    usual = (half - 1) * rows + rows // 2
    cut = (rows - quarter) // TILES
    for sem, less, more in ((right_send, before_wrap, before_last), (left_send, first_chip, after_first)):
        for case, count in (
            (less, usual - cut),
            (more, usual + cut),
            (jnp.logical_not(jnp.logical_or(less, more)), usual),
        ):

            @pl.when(case)
            def _(sem=sem, count=count):
                pltpu.make_async_copy(buf.at[:, pl.ds(0, count), :], buf.at[:, pl.ds(0, count), :], sem.at[0]).wait()

    sent = pl.ds(0, depth * rows)
    pltpu.make_async_copy(buf.at[:, sent, :], buf.at[:, sent, :], pair_send.at[0]).wait()
    pltpu.make_async_copy(landed, landed, term_send.at[0]).wait()


def put_out(screened_ref, sigma_ref, out_ref, sig_ref, sems):
    copies = [
        pltpu.make_async_copy(screened_ref, out_ref, sems.at[0]),
        pltpu.make_async_copy(sigma_ref, sig_ref, sems.at[1]),
    ]
    for copy in copies:
        copy.start()
    for copy in copies:
        copy.wait()


def local(devices, pair_elements, gmap, w_screened, coulomb):
    rows, pairs = pair_elements.shape
    width = pairs // TILES
    depth = devices // 2
    vmem = pl.BlockSpec(memory_space=pltpu.VMEM)
    hbm = pl.BlockSpec(memory_space=pl.ANY)
    screened, sigma = pl.pallas_call(
        functools.partial(kernel, devices),
        out_shape=(
            pltpu.VMEM((rows, pairs), jnp.float32),
            pltpu.VMEM((1, pairs // devices), jnp.float32),
        ),
        in_specs=[hbm, vmem, hbm, vmem],
        out_specs=(vmem, vmem),
        scratch_shapes=[
            pltpu.VMEM((TILES, devices * rows, width), jnp.float32),
            pltpu.VMEM((2, 2 * rows, rows), jnp.float32),
            pltpu.VMEM((5, rows, 2 * rows), jnp.bfloat16),
            pltpu.VMEM((5, rows, 2 * rows), jnp.bfloat16),
            pltpu.VMEM((TILES, 1, width), jnp.float32),
            pltpu.VMEM((TILES, 1, width), jnp.float32),
            pltpu.VMEM((pairs // 128, 1, 128), jnp.float32),
            pltpu.VMEM((devices - 1, 1, 128), jnp.float32),
            pltpu.SemaphoreType.DMA((depth, TILES)),
            pltpu.SemaphoreType.DMA((depth, TILES)),
            pltpu.SemaphoreType.DMA((1,)),
            pltpu.SemaphoreType.DMA((1,)),
            pltpu.SemaphoreType.DMA((1,)),
            pltpu.SemaphoreType.DMA((TILES,)),
            pltpu.SemaphoreType.DMA((2,)),
            pltpu.SemaphoreType.DMA((1,)),
            pltpu.SemaphoreType.DMA((1,)),
            pltpu.SemaphoreType.REGULAR,
            pltpu.SemaphoreType.DMA((4,)),
        ],
        compiler_params=pltpu.CompilerParams(
            collective_id=0, has_side_effects=True, vmem_limit_bytes=61 * 1024 * 1024
        ),
        name="ring_screen",
    )(pair_elements, gmap, w_screened, coulomb)
    screened, sigma = pl.pallas_call(
        put_out,
        out_shape=(
            jax.ShapeDtypeStruct((rows, pairs), jnp.float32),
            jax.ShapeDtypeStruct((1, pairs // devices), jnp.float32),
        ),
        in_specs=[vmem, vmem],
        out_specs=(hbm, hbm),
        scratch_shapes=[pltpu.SemaphoreType.DMA((2,))],
        compiler_params=pltpu.CompilerParams(vmem_limit_bytes=1024 * 1024),
        name="put_out",
    )(screened, sigma)
    return screened, sigma.reshape(pairs // devices)


def solution(mesh):
    in_specs = (
        P(("groups", "blk"), None),
        P(("groups", "blk")),
        P("groups", "blk"),
        P(("groups", "blk")),
    )
    out_specs = (P(("groups", "blk"), None), P(("groups", "blk")))
    body = functools.partial(local, mesh.shape["blk"])
    return jax.shard_map(body, mesh=mesh, in_specs=in_specs, out_specs=out_specs, check_vma=False)
```
